128 devices in a mesh: blk: 64 (over z_lo, x, y, core), grp: 2 (over z_hi).
Axes of the slice: x: 4, y: 4, z: 4 (z_hi: 2, z_lo: 2; z = z_hi * 2 + z_lo), core: 2. Of those that a mesh axis runs over, the one named last changes fastest.
Arguments:
- returns: float32 [512, 32768], P(None, ('blk', 'grp')), may hold values from -200 to 200
Outputs:
- correlation: bfloat16 [32768, 32768], P(('blk', 'grp'))
The draws below stay inside these ranges and needn't reach their ends.
All inputs are finite; a program needn't handle non-finite values.
Results may differ from the reference program's by a relative error of at most 0.0034.
Values may be sent and summed in bfloat16 or wider, within the bound.
A program may use at most 128 MiB of HBM per device.

```python
import math
import jax
import jax.numpy as jnp
from jax import lax

SER_DEV = 256
BARS = 512
SERIES = 32768


def draw_returns(key, part):
    subkeys = jax.random.split(key, 4)
    factor = jnp.clip(jax.random.normal(subkeys[0], (BARS, 1), jnp.float32), -4.0, 4.0)
    position = jnp.arange(SERIES, dtype=jnp.float32)[None, :] / SERIES
    loading = 0.5 + position + 0.3 * jnp.clip(jax.random.normal(subkeys[1], (1, SERIES), jnp.float32), -4.0, 4.0)
    volatility = jnp.exp(jax.random.uniform(subkeys[2], (1, SERIES), jnp.float32, math.log(0.3), math.log(3.0)))
    specific = 0.7 * jnp.clip(jax.random.normal(subkeys[3], (BARS, SERIES), jnp.float32), -4.0, 4.0)
    return (volatility * (factor * loading + specific)).astype(jnp.float32)


def setup_inputs(seed: int = 0) -> dict:
    arg_keys = jax.random.split(jax.random.key(seed), 2)
    returns = draw_returns(jax.random.fold_in(arg_keys[1], 71), 0)
    return {"returns": returns}


def reference(returns):
    market = lax.optimization_barrier(jnp.mean(returns, axis=1, keepdims=True))
    excess = returns - market
    deviation = excess - lax.optimization_barrier(jnp.mean(excess, axis=0, keepdims=True))
    inverse = lax.rsqrt(lax.optimization_barrier(jnp.mean(deviation * deviation, axis=0, keepdims=True)) + 1e-06) / math.sqrt(BARS)
    zscores = (deviation * inverse).astype(jnp.bfloat16)
    blocks = SERIES // SER_DEV
    columns = jnp.arange(SERIES, dtype=jnp.int32) // SER_DEV

    def row_block(row_index):
        block_rows = lax.dynamic_slice_in_dim(zscores, (row_index * SER_DEV).astype(jnp.int32), SER_DEV, 1)
        products = lax.dot_general(block_rows, zscores, (((0,), (0,)), ((), ())), preferred_element_type=jnp.float32)
        return jnp.where(columns[None, :] >= row_index, products, jnp.float32(0.0)).astype(jnp.bfloat16)
    stacked = lax.map(row_block, jnp.arange(blocks, dtype=jnp.int32))
    return stacked.reshape(SERIES, SERIES)
```

```python
import functools
import math

import jax
import jax.numpy as jnp
from jax import lax
from jax.experimental import pallas as pl
from jax.experimental.pallas import tpu as pltpu
from jax.sharding import PartitionSpec as P

MESH = pl.DeviceIdType.MESH
BARS = 512
SER = 256
HALF = SER // 2

TREE = [
    [(0, 1), (0, 1), (0, 1)], [(0, -1), (0, -1), (0, -1)], [(1, 1), (1, -1), (4, -1)],
    [(4, 1), (3, -1), (1, 1)], [(48, 1), (3, 1), (12, -1)], [(16, -1), (4, 1), (16, 1)],
    [(17, 1), (16, -1), (3, -1)], [(32, -1), (16, 1), (8, 1)], [(13, 1), (15, -1), (17, 1)],
    [(8, 1), (19, -1), (20, 1)], [(7, -1), (52, 1), (15, -1)], [(52, -1), (17, -1), (13, -1)],
    [(49, 1), (17, 1), (7, 1)], [(52, 1), (18, -1), (28, 1)], [(24, -1), (35, 1), (61, -1)],
    [(36, 1), (63, -1), (24, 1)], [(24, 1), (18, 1), (31, 1)], [(56, 1), (14, -1), (6, -1)],
    [(61, 1), (39, 1), (18, 1)], [(59, -1), (45, -1), (22, 1)], [(43, -1), (30, -1), (30, 1)],
]
SLOTS = len(TREE)


def build():
    place = {(0, 0, 0, 0): 0, (0, 0, 0, 1): 1}
    table = []
    for slot, row in enumerate(TREE):
        line = [None] * 6
        for axis, (parent, sign) in enumerate(row):
            for half in range(2):
                way = sign if half == 0 else -sign
                at = [parent % 4, parent // 4 % 4, parent // 16]
                if half:
                    at = [(-v) % 4 for v in at]
                to = list(at)
                to[axis] = (to[axis] + way) % 4
                d = 2 * axis + (way < 0)
                line[d] = (place[(*at, half)], tuple(to), half)
                place[(*to, half)] = 2 + 6 * slot + d
        table.append(line)
    return table


TABLE = build()


def kernel(
    r_ref, out_ref, zbuf, lhs, stage, rt, mtx, mrx,
    mtx_sem, mrx_sem, ltx_sem, lrx_sem, ztx_sem, zrx_sem, ttx_sem, trx_sem,
):
    blk = lax.axis_index("blk")
    grp = lax.axis_index("grp")
    core = blk % 2
    here = [blk // 8 % 4, blk // 2 % 4, grp * 2 + blk // 32]

    def device(at, c):
        x, y, z = at
        return (((z % 2) * 4 + x) * 4 + y) * 2 + c, z // 2

    def block(at, c):
        b, g = device(at, c)
        return b * 2 + g

    def along(axis, step):
        at = list(here)
        at[axis] = (at[axis] + step) % 4
        return device(at, core)

    mine = block(here, core)
    theirs = block(here, 1 - core)
    partner = device(here, 1 - core)
    ring = [[along(axis, step) for step in (1, 2, 3)] for axis in range(3)]

    def send(src, dst, send_sem, recv_sem, to):
        pltpu.make_async_remote_copy(
            src_ref=src, dst_ref=dst, send_sem=send_sem, recv_sem=recv_sem,
            device_id=to, device_id_type=MESH,
        ).start()

    def drain(ref, sem):
        pltpu.make_async_copy(ref, ref, sem).wait()

    barrier = pltpu.get_barrier_semaphore()
    peers = [partner] + [p for line in ring for p in line]
    for p in peers:
        pl.semaphore_signal(barrier, inc=1, device_id=p, device_id_type=MESH)

    turned = r_ref[...].T
    rt[...] = turned
    total = jnp.sum(turned, axis=0, keepdims=True)
    mtx[0] = total
    pl.semaphore_wait(barrier, len(peers))

    send(mtx.at[0], mrx.at[0], mtx_sem.at[0], mrx_sem.at[0], partner)
    drain(mrx.at[0], mrx_sem.at[0])
    total = total + mrx[0]
    for axis in range(3):
        mtx[axis + 1] = total
        for step in range(3):
            send(
                mtx.at[axis + 1], mrx.at[1 + 3 * axis + step],
                mtx_sem.at[axis + 1], mrx_sem.at[axis + 1], ring[axis][step],
            )
        drain(mrx.at[pl.ds(1 + 3 * axis, 3)], mrx_sem.at[axis + 1])
        total = total + (mrx[1 + 3 * axis] + mrx[2 + 3 * axis] + mrx[3 + 3 * axis])
    market = total / (SER * 128)

    excess = rt[...] - market
    deviation = excess - jnp.sum(excess, axis=1, keepdims=True) / BARS
    inverse = lax.rsqrt(
        jnp.sum(deviation * deviation, axis=1, keepdims=True) / BARS + 1e-6
    ) / math.sqrt(BARS)
    z = (deviation * inverse).astype(jnp.bfloat16)
    zbuf[0] = z[:HALF]
    zbuf[1] = z[HALF:]
    lhs[:SER] = z

    next_to = [along(d // 2, -1 if d % 2 else 1) for d in range(6)]

    def forward(slot):
        for d in range(6):
            piece, _, _ = TABLE[slot][d]
            send(
                zbuf.at[piece], zbuf.at[2 + 6 * slot + d],
                ztx_sem.at[slot], zrx_sem.at[slot], next_to[d],
            )

    forward(0)
    send(lhs.at[pl.ds(0, SER)], lhs.at[pl.ds(SER, SER)], ltx_sem, lrx_sem, partner)
    forward(1)

    def tiles(piece, source, half, where, send_sem, recv_sem):
        both = lax.dot_general(
            lhs[...], zbuf[piece], (((1,), (1,)), ((), ())),
            preferred_element_type=jnp.float32,
        )
        column = pl.ds(pl.multiple_of(source * SER + half * HALF, HALF), HALF)
        out_ref[:, column] = jnp.where(source >= mine, both[:SER], 0.0).astype(jnp.bfloat16)
        where[...] = jnp.where(source >= theirs, both[SER:], 0.0).astype(jnp.bfloat16)
        send(where, out_ref.at[:, column], send_sem, recv_sem, partner)

    drain(lhs.at[pl.ds(SER, SER)], lrx_sem)
    for half in range(2):
        tiles(half, mine, half, stage.at[2, half], ttx_sem.at[2], trx_sem.at[SLOTS])

    for slot in range(SLOTS):
        drain(zbuf.at[pl.ds(2 + 6 * slot, 6)], zrx_sem.at[slot])
        if slot + 2 < SLOTS:
            forward(slot + 2)
        bank = slot % 2
        if slot >= 2:
            drain(stage.at[bank], ttx_sem.at[bank])
        codes = [o[0] + 4 * o[1] + 16 * o[2] + 64 * h for _, o, h in TABLE[slot]]

        def one(d, carry, slot=slot, bank=bank, codes=codes):
            code = jnp.int32(codes[0])
            for other in range(1, 6):
                code = jnp.where(d == other, codes[other], code)
            offset = (code % 4, code // 4 % 4, code // 16 % 4)
            source = block([(here[a] + 4 - offset[a]) % 4 for a in range(3)], core)
            tiles(
                2 + 6 * slot + d, source, code // 64, stage.at[bank, d],
                ttx_sem.at[bank], trx_sem.at[slot],
            )
            return carry

        lax.fori_loop(0, 6, one, 0)

    for slot in range(SLOTS):
        drain(zbuf.at[pl.ds(2 + 6 * slot, 6)], ztx_sem.at[slot])
        drain(stage.at[0], trx_sem.at[slot])
    drain(stage.at[0], ttx_sem.at[0])
    drain(stage.at[1], ttx_sem.at[1])
    drain(stage.at[2, pl.ds(0, 2)], ttx_sem.at[2])
    drain(stage.at[2, pl.ds(0, 2)], trx_sem.at[SLOTS])
    drain(lhs.at[pl.ds(0, SER)], ltx_sem)
    drain(mtx.at[0], mtx_sem.at[0])
    for axis in range(3):
        drain(mrx.at[pl.ds(1 + 3 * axis, 3)], mtx_sem.at[axis + 1])


def shards(returns):
    dma = pltpu.SemaphoreType.DMA
    return pl.pallas_call(
        kernel,
        out_shape=pltpu.VMEM((SER, 128 * SER), jnp.bfloat16),
        in_specs=[pl.BlockSpec(memory_space=pltpu.VMEM)],
        out_specs=pl.BlockSpec(memory_space=pltpu.VMEM),
        scratch_shapes=[
            pltpu.VMEM((128, HALF, BARS), jnp.bfloat16),
            pltpu.VMEM((2 * SER, BARS), jnp.bfloat16),
            pltpu.VMEM((3, 6, SER, HALF), jnp.bfloat16),
            pltpu.VMEM((SER, BARS), jnp.float32),
            pltpu.VMEM((4, 1, BARS), jnp.float32),
            pltpu.VMEM((10, 1, BARS), jnp.float32),
            dma((4,)), dma((4,)), dma, dma,
            dma((SLOTS,)), dma((SLOTS,)), dma((3,)), dma((SLOTS + 1,)),
        ],
        compiler_params=pltpu.CompilerParams(
            collective_id=0, has_side_effects=True, vmem_limit_bytes=30 * 2**20
        ),
    )(returns)


def solution(mesh):
    axes = ("blk", "grp")
    return jax.shard_map(
        shards, mesh=mesh, in_specs=(P(None, axes),), out_specs=P(axes, None), check_vma=False
    )
```

```python
import functools
import math

import jax
import jax.numpy as jnp
from jax import lax
from jax.experimental import pallas as pl
from jax.experimental.pallas import tpu as pltpu
from jax.sharding import PartitionSpec as P

MESH = pl.DeviceIdType.MESH
BARS = 512
SER = 256
HALF = SER // 2
PARTS = 8

TREE = [
    [(0, 1), (0, 1), (0, 1)], [(0, -1), (0, -1), (0, -1)], [(1, 1), (1, -1), (4, -1)],
    [(4, 1), (3, -1), (1, 1)], [(48, 1), (3, 1), (12, -1)], [(16, -1), (4, 1), (16, 1)],
    [(17, 1), (16, -1), (3, -1)], [(32, -1), (16, 1), (8, 1)], [(13, 1), (15, -1), (17, 1)],
    [(8, 1), (19, -1), (20, 1)], [(7, -1), (52, 1), (15, -1)], [(52, -1), (17, -1), (13, -1)],
    [(49, 1), (17, 1), (7, 1)], [(52, 1), (18, -1), (28, 1)], [(24, -1), (35, 1), (61, -1)],
    [(36, 1), (63, -1), (24, 1)], [(24, 1), (18, 1), (31, 1)], [(56, 1), (14, -1), (6, -1)],
    [(61, 1), (39, 1), (18, 1)], [(59, -1), (45, -1), (22, 1)], [(43, -1), (30, -1), (30, 1)],
]
SLOTS = len(TREE)


def build():
    place = {(0, 0, 0, 0): 0, (0, 0, 0, 1): 1}
    table = []
    for slot, row in enumerate(TREE):
        line = [None] * 6
        for axis, (parent, sign) in enumerate(row):
            for half in range(2):
                way = sign if half == 0 else -sign
                at = [parent % 4, parent // 4 % 4, parent // 16]
                if half:
                    at = [(-v) % 4 for v in at]
                to = list(at)
                to[axis] = (to[axis] + way) % 4
                d = 2 * axis + (way < 0)
                line[d] = (place[(*at, half)], tuple(to), half)
                place[(*to, half)] = 2 + 6 * slot + d
        table.append(line)
    return table


TABLE = build()


def kernel(
    r_ref, out_ref, zbuf, lhs, stage, inp, rt, raw, mrx,
    in_sem, mtx_sem, mrx_sem, wtx_sem, wrx_sem, ltx_sem, lrx_sem, ztx_sem, zrx_sem, ttx_sem, trx_sem,
):
    load = pltpu.make_async_copy(r_ref, inp, in_sem)
    load.start()
    blk = lax.axis_index("blk")
    grp = lax.axis_index("grp")
    core = blk % 2
    here = [blk // 8 % 4, blk // 2 % 4, grp * 2 + blk // 32]

    def device(at, c):
        x, y, z = at
        return (((z % 2) * 4 + x) * 4 + y) * 2 + c, z // 2

    def block(at, c):
        b, g = device(at, c)
        return b * 2 + g

    def along(axis, step, c):
        at = list(here)
        at[axis] = (at[axis] + step) % 4
        return device(at, c)

    mine = block(here, core)
    theirs = block(here, 1 - core)
    partner = device(here, 1 - core)
    next_to = [along(d // 2, -1 if d % 2 else 1, core) for d in range(6)]

    def send(src, dst, send_sem, recv_sem, to):
        pltpu.make_async_remote_copy(
            src_ref=src, dst_ref=dst, send_sem=send_sem, recv_sem=recv_sem,
            device_id=to, device_id_type=MESH,
        ).start()

    def drain(ref, sem):
        pltpu.make_async_copy(ref, ref, sem).wait()

    barrier = pltpu.get_barrier_semaphore()
    peers = [partner]
    for axis in range(3):
        for step in (2, 1, 3):
            peers.append(along(axis, step, core))
            if axis != 1:
                peers.append(along(axis, step, 1 - core))
    for p in peers:
        pl.semaphore_signal(barrier, inc=1, device_id=p, device_id_type=MESH)

    load.wait()
    turned = inp[...].T
    rt[...] = turned
    first = here[0] * 2 + core
    mrx[first] = jnp.sum(turned, axis=0, keepdims=True)
    pl.semaphore_wait(barrier, len(peers))

    def bulk(d):
        send(rt.at[pl.ds((d % 2) * HALF, HALF)], raw.at[d], wtx_sem, wrx_sem, next_to[d])

    def ring_sum(low, count):
        total = mrx[low]
        for n in range(1, count):
            total = total + mrx[low + n]
        return total

    def sum_to(slot, low, axis, c, phase):
        for step in (2, 1, 3):
            send(mrx.at[slot], mrx.at[slot], mtx_sem.at[phase], mrx_sem.at[phase], along(axis, step, c))

    @pl.when(core == 0)
    def _():
        send(mrx.at[first], mrx.at[first], mtx_sem.at[0], mrx_sem.at[0], partner)
        sum_to(first, 0, 0, 1, 0)
        for d in range(6):
            bulk(d)
        drain(mrx.at[pl.ds(12, 4)], mrx_sem.at[2])
        drain(mrx.at[pl.ds(0, 4)], mtx_sem.at[0])

    @pl.when(core == 1)
    def _():
        sum_to(first, 0, 0, 1, 0)
        for d in (0, 1, 4, 5):
            bulk(d)
        drain(mrx.at[pl.ds(0, 7)], mrx_sem.at[0])
        second = 8 + here[1]
        mrx[second] = ring_sum(0, 8)
        sum_to(second, 8, 1, 1, 1)
        bulk(2)
        bulk(3)
        drain(mrx.at[pl.ds(8, 3)], mrx_sem.at[1])
        third = 12 + here[2]
        mrx[third] = ring_sum(8, 4)
        sum_to(third, 12, 2, 1, 2)
        sum_to(third, 12, 2, 0, 2)
        send(mrx.at[third], mrx.at[third], mtx_sem.at[2], mrx_sem.at[2], partner)
        drain(mrx.at[pl.ds(12, 3)], mrx_sem.at[2])
        drain(mrx.at[pl.ds(0, 3)], mtx_sem.at[0])
        drain(mrx.at[pl.ds(8, 3)], mtx_sem.at[1])
        drain(mrx.at[pl.ds(0, 7)], mtx_sem.at[2])

    market = ring_sum(12, 4) / (SER * 128)

    def zscore(series):
        excess = series - market
        deviation = excess - jnp.sum(excess, axis=1, keepdims=True) / BARS
        inverse = lax.rsqrt(
            jnp.sum(deviation * deviation, axis=1, keepdims=True) / BARS + 1e-6
        ) / math.sqrt(BARS)
        return (deviation * inverse).astype(jnp.bfloat16)

    def forward(slot, d):
        send(
            zbuf.at[TABLE[slot][d][0]], zbuf.at[2 + 6 * slot + d],
            ztx_sem.at[slot], zrx_sem.at[slot], next_to[d],
        )

    for half in range(2):
        z = zscore(rt[half * HALF:(half + 1) * HALF])
        zbuf[half] = z
        lhs[half * HALF:(half + 1) * HALF] = z
        for d in range(6):
            if TABLE[1][d][0] == half:
                forward(1, d)
    send(lhs.at[pl.ds(0, SER)], lhs.at[pl.ds(SER, SER)], ltx_sem, lrx_sem, partner)
    drain(raw, wrx_sem)

    def from_raw(d, carry):
        zbuf[2 + d] = zscore(raw[d])
        return carry

    lax.fori_loop(0, 6, from_raw, 0)
    for d in range(6):
        forward(2, d)

    def tiles(piece, source, half, where, send_sem, recv_sem):
        both = lax.dot_general(
            lhs[...], zbuf[piece], (((1,), (1,)), ((), ())),
            preferred_element_type=jnp.float32,
        )
        column = pl.ds(pl.multiple_of(source * SER + half * HALF, HALF), HALF)
        out_ref[:, column] = jnp.where(source >= mine, both[:SER], 0.0).astype(jnp.bfloat16)
        where[...] = jnp.where(source >= theirs, both[SER:], 0.0).astype(jnp.bfloat16)
        send(where, out_ref.at[:, column], send_sem, recv_sem, partner)

    drain(lhs.at[pl.ds(SER, SER)], lrx_sem)
    for half in range(2):
        tiles(half, mine, half, stage.at[2, half], ttx_sem.at[2], trx_sem.at[SLOTS])

    for slot in range(SLOTS):
        if slot:
            drain(zbuf.at[pl.ds(2 + 6 * slot, 6)], zrx_sem.at[slot])
            for d in range(6 if slot + 2 < SLOTS else 0):
                forward(slot + 2, d)
        bank = slot % 2
        if slot >= 2:
            drain(stage.at[bank], ttx_sem.at[bank])
        codes = [o[0] + 4 * o[1] + 16 * o[2] + 64 * h for _, o, h in TABLE[slot]]

        def one(d, carry, slot=slot, bank=bank, codes=codes):
            code = jnp.int32(codes[0])
            for other in range(1, 6):
                code = jnp.where(d == other, codes[other], code)
            offset = (code % 4, code // 4 % 4, code // 16 % 4)
            source = block([(here[a] + 4 - offset[a]) % 4 for a in range(3)], core)
            tiles(
                2 + 6 * slot + d, source, code // 64, stage.at[bank, d],
                ttx_sem.at[bank], trx_sem.at[slot],
            )
            return carry

        lax.fori_loop(0, 6, one, 0)

    for slot in range(SLOTS):
        if slot:
            drain(zbuf.at[pl.ds(2 + 6 * slot, 6)], ztx_sem.at[slot])
        drain(stage.at[0], trx_sem.at[slot])
    drain(stage.at[0], ttx_sem.at[0])
    drain(stage.at[1], ttx_sem.at[1])
    drain(stage.at[2, pl.ds(0, 2)], ttx_sem.at[2])
    drain(stage.at[2, pl.ds(0, 2)], trx_sem.at[SLOTS])
    drain(lhs.at[pl.ds(0, SER)], ltx_sem)
    drain(raw, wtx_sem)


def write_out(held_ref, out_ref, sem):
    rows = SER // PARTS
    copies = []
    for n in range(PARTS):
        part = pl.ds(n * rows, rows)
        copies.append(pltpu.make_async_copy(held_ref.at[part], out_ref.at[part], sem.at[n]))
        copies[n].start()
    for copy in copies:
        copy.wait()


def shards(returns):
    dma = pltpu.SemaphoreType.DMA
    held = pl.pallas_call(
        kernel,
        out_shape=pltpu.VMEM((SER, 128 * SER), jnp.bfloat16),
        in_specs=[pl.BlockSpec(memory_space=pltpu.HBM)],
        out_specs=pl.BlockSpec(memory_space=pltpu.VMEM),
        scratch_shapes=[
            pltpu.VMEM((128, HALF, BARS), jnp.bfloat16),
            pltpu.VMEM((2 * SER, BARS), jnp.bfloat16),
            pltpu.VMEM((3, 6, SER, HALF), jnp.bfloat16),
            pltpu.VMEM((BARS, SER), jnp.float32),
            pltpu.VMEM((SER, BARS), jnp.float32),
            pltpu.VMEM((6, HALF, BARS), jnp.float32),
            pltpu.VMEM((16, 1, BARS), jnp.float32),
            dma, dma((3,)), dma((3,)), dma, dma, dma, dma,
            dma((SLOTS,)), dma((SLOTS,)), dma((3,)), dma((SLOTS + 1,)),
        ],
        compiler_params=pltpu.CompilerParams(
            collective_id=0, has_side_effects=True, vmem_limit_bytes=30 * 2**20
        ),
    )(pltpu.with_memory_space_constraint(returns, pltpu.HBM))
    return pl.pallas_call(
        write_out,
        out_shape=jax.ShapeDtypeStruct((SER, 128 * SER), jnp.bfloat16),
        in_specs=[pl.BlockSpec(memory_space=pltpu.VMEM)],
        out_specs=pl.BlockSpec(memory_space=pl.ANY),
        scratch_shapes=[dma((PARTS,))],
        compiler_params=pltpu.CompilerParams(vmem_limit_bytes=2**20),
    )(pltpu.with_memory_space_constraint(held, pltpu.VMEM))


def solution(mesh):
    axes = ("blk", "grp")
    return jax.shard_map(
        shards, mesh=mesh, in_specs=(P(None, axes),), out_specs=P(axes, None), check_vma=False
    )
```

```python
import functools
import math

import jax
import jax.numpy as jnp
from jax import lax
from jax.experimental import pallas as pl
from jax.experimental.pallas import tpu as pltpu
from jax.sharding import PartitionSpec as P

MESH = pl.DeviceIdType.MESH
BARS = 512
SER = 256
HALF = SER // 2
PARTS = 8
DEPTH = 4
QUARTER = HALF // 2
CHUNKS = 4

TREE = [
    [(0, 1), (0, 1), (0, 1)], [(0, -1), (0, -1), (0, -1)], [(1, 1), (1, -1), (4, -1)],
    [(4, 1), (3, -1), (1, 1)], [(48, 1), (3, 1), (12, -1)], [(16, -1), (4, 1), (16, 1)],
    [(17, 1), (16, -1), (3, -1)], [(32, -1), (16, 1), (8, 1)], [(13, 1), (15, -1), (17, 1)],
    [(8, 1), (19, -1), (20, 1)], [(7, -1), (52, 1), (15, -1)], [(52, -1), (17, -1), (13, -1)],
    [(49, 1), (17, 1), (7, 1)], [(52, 1), (18, -1), (28, 1)], [(24, -1), (35, 1), (61, -1)],
    [(36, 1), (63, -1), (24, 1)], [(24, 1), (18, 1), (31, 1)], [(56, 1), (14, -1), (6, -1)],
    [(61, 1), (39, 1), (18, 1)], [(59, -1), (45, -1), (22, 1)], [(43, -1), (30, -1), (30, 1)],
]
SLOTS = len(TREE)


def build():
    place = {(0, 0, 0, 0): 0, (0, 0, 0, 1): 1}
    table = []
    for slot, row in enumerate(TREE):
        line = [None] * 6
        for axis, (parent, sign) in enumerate(row):
            for half in range(2):
                way = sign if half == 0 else -sign
                at = [parent % 4, parent // 4 % 4, parent // 16]
                if half:
                    at = [(-v) % 4 for v in at]
                to = list(at)
                to[axis] = (to[axis] + way) % 4
                d = 2 * axis + (way < 0)
                line[d] = (place[(*at, half)], tuple(to), half)
                place[(*to, half)] = 2 + 6 * slot + d
        table.append(line)
    return table


TABLE = build()


def issue_plan():
    plan = [[] for _ in range(SLOTS)]
    when = [0] * 6
    for slot in range(2, SLOTS):
        for d in range(6):
            when[d] = max((TABLE[slot][d][0] - 2) // 6, when[d], slot - DEPTH)
            plan[when[d]].append((slot, d))
    return plan


PLAN = issue_plan()


def kernel(
    r_ref, out_ref, zbuf, lhs, stage, inp, rt, raw, early, mrx,
    in_sem, mtx_sem, mrx_sem, wtx_sem, wrx_sem, ltx_sem, lrx_sem, ztx_sem, zrx_sem, ttx_sem, trx_sem,
):
    span = BARS // CHUNKS
    loads = []
    for q in range(CHUNKS):
        part = pl.ds(q * span, span)
        loads.append(pltpu.make_async_copy(r_ref.at[part], inp.at[part], in_sem.at[q]))
        loads[q].start()
    blk = lax.axis_index("blk")
    grp = lax.axis_index("grp")
    core = blk % 2
    here = [blk // 8 % 4, blk // 2 % 4, grp * 2 + blk // 32]

    def device(at, c):
        x, y, z = at
        return (((z % 2) * 4 + x) * 4 + y) * 2 + c, z // 2

    def block(at, c):
        b, g = device(at, c)
        return b * 2 + g

    def away(x, y, z, c):
        return device([(here[0] + x) % 4, (here[1] + y) % 4, (here[2] + z) % 4], c)

    mine = block(here, core)
    theirs = block(here, 1 - core)
    partner = device(here, 1 - core)
    steps = [(1, 0, 0), (3, 0, 0), (0, 1, 0), (0, 3, 0), (0, 0, 1), (0, 0, 3)]
    next_to = [away(*step, core) for step in steps]
    ring = [(x, 0, 0) for x in (2, 1, 3)]
    plane = [(0, y, z) for y in (2, 1, 3, 0) for z in (2, 1, 3, 0) if (y, z) != (0, 0)]

    def send(src, dst, send_sem, recv_sem, to):
        pltpu.make_async_remote_copy(
            src_ref=src, dst_ref=dst, send_sem=send_sem, recv_sem=recv_sem,
            device_id=to, device_id_type=MESH,
        ).start()

    def drain(ref, sem):
        pltpu.make_async_copy(ref, ref, sem).wait()

    barrier = pltpu.get_barrier_semaphore()

    def greet(devices):
        for to in devices:
            pl.semaphore_signal(barrier, inc=1, device_id=to, device_id_type=MESH)
        return len(devices)

    zero_peers = [partner] + [away(*o, 1 - core) for o in ring] + next_to
    one_peers = zero_peers[:4] + [away(*o, core) for o in plane + ring]

    @pl.when(core == 0)
    def _():
        greet(zero_peers)

    @pl.when(core == 1)
    def _():
        greet(one_peers)

    first = here[0] * 2 + core
    for q in range(CHUNKS):
        loads[q].wait()
        bars = inp[q * span:(q + 1) * span]
        pairs = bars[:, :HALF] + bars[:, HALF:]
        mrx[first, :, q * span:(q + 1) * span] = jnp.sum(pairs.T, axis=0, keepdims=True)

    def add_up(low, count):
        total = mrx[low]
        for n in range(1, count):
            total = total + mrx[low + n]
        return total

    def raw_first(d):
        send(rt.at[pl.ds((d % 2) * HALF, HALF)], raw.at[d], wtx_sem.at[0], wrx_sem.at[0], next_to[d])

    def raw_second(d):
        rows = pl.ds((1 - d % 2) * HALF, QUARTER)
        send(rt.at[rows], early.at[d], wtx_sem.at[1], wrx_sem.at[1], next_to[d])

    def turn():
        for q in range(CHUNKS):
            rt[:, q * span:(q + 1) * span] = inp[q * span:(q + 1) * span].T

    @pl.when(core == 0)
    def _():
        pl.semaphore_wait(barrier, len(zero_peers))
        send(mrx.at[first], mrx.at[first], mtx_sem.at[0], mrx_sem.at[0], partner)
        for o in ring:
            send(mrx.at[first], mrx.at[first], mtx_sem.at[0], mrx_sem.at[0], away(*o, 1))
        turn()
        for d in range(6):
            raw_first(d)
        for d in range(6):
            raw_second(d)
        drain(mrx.at[24], mrx_sem.at[2])
        drain(mrx.at[pl.ds(0, 4)], mtx_sem.at[0])

    @pl.when(core == 1)
    def _():
        pl.semaphore_wait(barrier, len(one_peers))
        for o in ring:
            send(mrx.at[first], mrx.at[first], mtx_sem.at[0], mrx_sem.at[0], away(*o, 1))
        turn()
        for d in (2, 3, 4, 5):
            raw_second(d)
        for d in (0, 1):
            raw_first(d)
            raw_second(d)
        drain(mrx.at[pl.ds(0, 7)], mrx_sem.at[0])
        second = 8 + here[1] * 4 + here[2]
        mrx[second] = add_up(0, 8)
        for o in plane:
            send(mrx.at[second], mrx.at[second], mtx_sem.at[1], mrx_sem.at[1], away(*o, 1))
        for d in (2, 3, 4, 5):
            raw_first(d)
        drain(mrx.at[pl.ds(8, 15)], mrx_sem.at[1])
        mrx[24] = add_up(8, 16)
        send(mrx.at[24], mrx.at[24], mtx_sem.at[2], mrx_sem.at[2], partner)
        drain(mrx.at[pl.ds(0, 3)], mtx_sem.at[0])
        drain(mrx.at[pl.ds(8, 15)], mtx_sem.at[1])
        drain(mrx.at[24], mtx_sem.at[2])

    market = mrx[24] / (SER * 128)

    def zscore(series):
        excess = series - market
        deviation = excess - jnp.sum(excess, axis=1, keepdims=True) / BARS
        inverse = lax.rsqrt(
            jnp.sum(deviation * deviation, axis=1, keepdims=True) / BARS + 1e-6
        ) / math.sqrt(BARS)
        return (deviation * inverse).astype(jnp.bfloat16)

    def forward(slot, d):
        send(
            zbuf.at[TABLE[slot][d][0]], zbuf.at[2 + 6 * slot + d],
            ztx_sem.at[slot], zrx_sem.at[slot], next_to[d],
        )

    late = pl.ds(QUARTER, QUARTER)
    for half in range(2):
        z = zscore(rt[half * HALF:(half + 1) * HALF])
        zbuf[half] = z
        lhs[half * HALF:(half + 1) * HALF] = z
        for d in range(6):
            if TABLE[1][d][0] == half:
                send(
                    zbuf.at[half, late], zbuf.at[8 + d, late],
                    ztx_sem.at[1], zrx_sem.at[1], next_to[d],
                )
    send(lhs.at[pl.ds(0, SER)], lhs.at[pl.ds(SER, SER)], ltx_sem, lrx_sem, partner)

    drain(raw, wrx_sem.at[0])
    waiting = list(PLAN[0])
    for n in range(6):
        zbuf[2 + n] = zscore(raw[n])
        held = set()
        for slot, d in list(waiting):
            if d in held or TABLE[slot][d][0] > 2 + n:
                held.add(d)
            else:
                forward(slot, d)
                waiting.remove((slot, d))
    drain(early, wrx_sem.at[1])

    def from_early(d, carry):
        zbuf[8 + d, :QUARTER] = zscore(early[d])
        return carry

    lax.fori_loop(0, 6, from_early, 0)

    def tiles(piece, sources, halves, where, send_sem, recv_sem):
        both = lax.dot_general(
            lhs[...], zbuf[pl.ds(piece, 2)].reshape(SER, BARS), (((1,), (1,)), ((), ())),
            preferred_element_type=jnp.float32,
        )
        for n in range(2):
            part = both[:, n * HALF:(n + 1) * HALF]
            column = pl.ds(pl.multiple_of(sources[n] * SER + halves[n] * HALF, HALF), HALF)
            where[n] = jnp.where(sources[n] >= theirs, part[SER:], 0.0).astype(jnp.bfloat16)
            out_ref[:, column] = jnp.where(sources[n] >= mine, part[:SER], 0.0).astype(jnp.bfloat16)
            send(where.at[n], out_ref.at[:, column], send_sem, recv_sem, partner)

    def landed(slot):
        if slot == 1:
            return zbuf.at[pl.ds(8, 6), late]
        return zbuf.at[pl.ds(2 + 6 * slot, 6)]

    drain(lhs.at[pl.ds(SER, SER)], lrx_sem)
    tiles(
        0, (mine, mine), (0, 1), stage.at[2, pl.ds(0, 2)], ttx_sem.at[2], trx_sem.at[SLOTS]
    )

    for slot in range(SLOTS):
        if slot:
            drain(landed(slot), zrx_sem.at[slot])
            for later, d in PLAN[slot]:
                forward(later, d)
        bank = slot % 2
        if slot >= 2:
            drain(stage.at[bank], ttx_sem.at[bank])
        codes = [o[0] + 4 * o[1] + 16 * o[2] + 64 * h for _, o, h in TABLE[slot]]

        def one(axis, carry, slot=slot, bank=bank, codes=codes):
            sources, halves = [], []
            for n in range(2):
                code = jnp.where(axis == 0, codes[n], jnp.where(axis == 1, codes[2 + n], codes[4 + n]))
                offset = (code % 4, code // 4 % 4, code // 16 % 4)
                sources.append(block([(here[a] + 4 - offset[a]) % 4 for a in range(3)], core))
                halves.append(code // 64)
            tiles(
                2 + 6 * slot + 2 * axis, sources, halves, stage.at[bank, pl.ds(2 * axis, 2)],
                ttx_sem.at[bank], trx_sem.at[slot],
            )
            return carry

        lax.fori_loop(0, 3, one, 0)

    for slot in range(SLOTS):
        if slot:
            drain(landed(slot), ztx_sem.at[slot])
        drain(stage.at[0], trx_sem.at[slot])
    drain(stage.at[0], ttx_sem.at[0])
    drain(stage.at[1], ttx_sem.at[1])
    drain(stage.at[2, pl.ds(0, 2)], ttx_sem.at[2])
    drain(stage.at[2, pl.ds(0, 2)], trx_sem.at[SLOTS])
    drain(lhs.at[pl.ds(0, SER)], ltx_sem)
    drain(raw, wtx_sem.at[0])
    drain(early, wtx_sem.at[1])


def write_out(held_ref, out_ref, sem):
    rows = SER // PARTS
    copies = []
    for n in range(PARTS):
        part = pl.ds(n * rows, rows)
        copies.append(pltpu.make_async_copy(held_ref.at[part], out_ref.at[part], sem.at[n]))
        copies[n].start()
    for copy in copies:
        copy.wait()


def shards(returns):
    dma = pltpu.SemaphoreType.DMA
    held = pl.pallas_call(
        kernel,
        out_shape=pltpu.VMEM((SER, 128 * SER), jnp.bfloat16),
        in_specs=[pl.BlockSpec(memory_space=pltpu.HBM)],
        out_specs=pl.BlockSpec(memory_space=pltpu.VMEM),
        scratch_shapes=[
            pltpu.VMEM((128, HALF, BARS), jnp.bfloat16),
            pltpu.VMEM((2 * SER, BARS), jnp.bfloat16),
            pltpu.VMEM((3, 6, SER, HALF), jnp.bfloat16),
            pltpu.VMEM((BARS, SER), jnp.float32),
            pltpu.VMEM((SER, BARS), jnp.float32),
            pltpu.VMEM((6, HALF, BARS), jnp.float32),
            pltpu.VMEM((6, QUARTER, BARS), jnp.float32),
            pltpu.VMEM((25, 1, BARS), jnp.float32),
            dma((CHUNKS,)), dma((3,)), dma((3,)), dma((2,)), dma((2,)), dma, dma,
            dma((SLOTS,)), dma((SLOTS,)), dma((3,)), dma((SLOTS + 1,)),
        ],
        compiler_params=pltpu.CompilerParams(
            collective_id=0, has_side_effects=True, vmem_limit_bytes=30 * 2**20
        ),
    )(pltpu.with_memory_space_constraint(returns, pltpu.HBM))
    return pl.pallas_call(
        write_out,
        out_shape=jax.ShapeDtypeStruct((SER, 128 * SER), jnp.bfloat16),
        in_specs=[pl.BlockSpec(memory_space=pltpu.VMEM)],
        out_specs=pl.BlockSpec(memory_space=pl.ANY),
        scratch_shapes=[dma((PARTS,))],
        compiler_params=pltpu.CompilerParams(vmem_limit_bytes=2**20),
    )(pltpu.with_memory_space_constraint(held, pltpu.VMEM))


def solution(mesh):
    axes = ("blk", "grp")
    return jax.shard_map(
        shards, mesh=mesh, in_specs=(P(None, axes),), out_specs=P(axes, None), check_vma=False
    )
```

```python
import functools
import math

import jax
import jax.numpy as jnp
from jax import lax
from jax.experimental import pallas as pl
from jax.experimental.pallas import tpu as pltpu
from jax.sharding import PartitionSpec as P

MESH = pl.DeviceIdType.MESH
BARS = 512
SER = 256
HALF = SER // 2
PARTS = 8
DEPTH = 4
BEHIND = 3
QUARTER = HALF // 2
CHUNKS = 4

TREE = [
    [(0, 1), (0, 1), (0, 1)], [(0, -1), (0, -1), (0, -1)], [(1, 1), (1, -1), (4, -1)],
    [(4, 1), (3, -1), (1, 1)], [(48, 1), (3, 1), (12, -1)], [(16, -1), (4, 1), (16, 1)],
    [(17, 1), (16, -1), (3, -1)], [(32, -1), (16, 1), (8, 1)], [(13, 1), (15, -1), (17, 1)],
    [(8, 1), (19, -1), (20, 1)], [(7, -1), (52, 1), (15, -1)], [(52, -1), (17, -1), (13, -1)],
    [(49, 1), (17, 1), (7, 1)], [(52, 1), (18, -1), (28, 1)], [(24, -1), (35, 1), (61, -1)],
    [(36, 1), (63, -1), (24, 1)], [(24, 1), (18, 1), (31, 1)], [(56, 1), (14, -1), (6, -1)],
    [(61, 1), (39, 1), (18, 1)], [(59, -1), (45, -1), (22, 1)], [(43, -1), (30, -1), (30, 1)],
]
SLOTS = len(TREE)


def build():
    place = {(0, 0, 0, 0): 0, (0, 0, 0, 1): 1}
    table = []
    for slot, row in enumerate(TREE):
        line = [None] * 6
        for axis, (parent, sign) in enumerate(row):
            for half in range(2):
                way = sign if half == 0 else -sign
                at = [parent % 4, parent // 4 % 4, parent // 16]
                if half:
                    at = [(-v) % 4 for v in at]
                to = list(at)
                to[axis] = (to[axis] + way) % 4
                d = 2 * axis + (way < 0)
                line[d] = (place[(*at, half)], tuple(to), half)
                place[(*to, half)] = 2 + 6 * slot + d
        table.append(line)
    return table


TABLE = build()


def issue_plan():
    plan = [[] for _ in range(SLOTS)]
    when = [0] * 6
    for slot in range(2, SLOTS):
        for d in range(6):
            when[d] = max((TABLE[slot][d][0] - 2) // 6, when[d], slot - DEPTH)
            plan[when[d]].append((slot, d))
    return plan


PLAN = issue_plan()


def kernel(
    r_ref, out_ref, zbuf, lhs, stage, inp, rt, raw, early, mrx,
    in_sem, mtx_sem, mrx_sem, wtx_sem, wrx_sem, etx_sem, erx_sem,
    ltx_sem, lrx_sem, ztx_sem, zrx_sem, ttx_sem, trx_sem,
):
    span = BARS // CHUNKS
    loads = []
    for q in range(CHUNKS):
        part = pl.ds(q * span, span)
        loads.append(pltpu.make_async_copy(r_ref.at[part], inp.at[part], in_sem.at[q]))
        loads[q].start()
    blk = lax.axis_index("blk")
    grp = lax.axis_index("grp")
    core = blk % 2
    here = [blk // 8 % 4, blk // 2 % 4, grp * 2 + blk // 32]

    def device(at, c):
        x, y, z = at
        return (((z % 2) * 4 + x) * 4 + y) * 2 + c, z // 2

    def block(at, c):
        b, g = device(at, c)
        return b * 2 + g

    def away(x, y, z, c):
        return device([(here[0] + x) % 4, (here[1] + y) % 4, (here[2] + z) % 4], c)

    mine = block(here, core)
    theirs = block(here, 1 - core)
    partner = device(here, 1 - core)
    steps = [(1, 0, 0), (3, 0, 0), (0, 1, 0), (0, 3, 0), (0, 0, 1), (0, 0, 3)]
    next_to = [away(*step, core) for step in steps]
    ring = [(x, 0, 0) for x in (2, 1, 3)]
    plane = [(0, y, z) for y in (2, 1, 3, 0) for z in (2, 1, 3, 0) if (y, z) != (0, 0)]

    def send(src, dst, send_sem, recv_sem, to):
        pltpu.make_async_remote_copy(
            src_ref=src, dst_ref=dst, send_sem=send_sem, recv_sem=recv_sem,
            device_id=to, device_id_type=MESH,
        ).start()

    def drain(ref, sem):
        pltpu.make_async_copy(ref, ref, sem).wait()

    barrier = pltpu.get_barrier_semaphore()

    def greet(devices):
        for to in devices:
            pl.semaphore_signal(barrier, inc=1, device_id=to, device_id_type=MESH)
        return len(devices)

    ring_peers = [partner] + [away(*o, 1 - core) for o in ring]
    one_peers = [away(*o, 1) for o in plane]

    @pl.when(core == 0)
    def _():
        greet(ring_peers + next_to + one_peers)

    @pl.when(core == 1)
    def _():
        greet(ring_peers + one_peers + [away(*o, core) for o in ring])

    first = here[0] * 2 + core
    for q in range(CHUNKS):
        loads[q].wait()
        bars = inp[q * span:(q + 1) * span]
        pairs = bars[:, :HALF] + bars[:, HALF:]
        mrx[first, :, q * span:(q + 1) * span] = jnp.sum(pairs.T, axis=0, keepdims=True)

    def add_up(low, count):
        total = mrx[low]
        for n in range(1, count):
            total = total + mrx[low + n]
        return total

    def raw_first(d):
        send(rt.at[pl.ds((d % 2) * HALF, HALF)], raw.at[d], wtx_sem, wrx_sem, next_to[d])

    def raw_part(d, n):
        rows = pl.ds((d % 2) * HALF + n * QUARTER, QUARTER)
        send(rt.at[rows], raw.at[d, pl.ds(n * QUARTER, QUARTER)], wtx_sem, wrx_sem, next_to[d])

    def raw_second(d):
        rows = pl.ds((1 - d % 2) * HALF, QUARTER)
        send(rt.at[rows], early.at[d], etx_sem, erx_sem, next_to[d])

    def turn():
        for q in range(CHUNKS):
            rt[:, q * span:(q + 1) * span] = inp[q * span:(q + 1) * span].T
        series = rt[...]
        rt[...] = series - jnp.sum(series, axis=1, keepdims=True) / BARS

    @pl.when(core == 0)
    def _():
        pl.semaphore_wait(barrier, 4 + 6)
        send(mrx.at[first], mrx.at[first], mtx_sem.at[0], mrx_sem.at[0], partner)
        for o in ring:
            send(mrx.at[first], mrx.at[first], mtx_sem.at[0], mrx_sem.at[0], away(*o, 1))
        turn()
        for d in range(6):
            raw_first(d)
        for d in range(6):
            raw_second(d)
        drain(mrx.at[pl.ds(8, 16)], mrx_sem.at[1])
        drain(mrx.at[pl.ds(0, 4)], mtx_sem.at[0])

    @pl.when(core == 1)
    def _():
        pl.semaphore_wait(barrier, 4 + 15 + 3 + 15)
        for o in ring:
            send(mrx.at[first], mrx.at[first], mtx_sem.at[0], mrx_sem.at[0], away(*o, 1))
        turn()
        for d in (2, 3, 4, 5):
            raw_part(d, 0)
        for d in (0, 1):
            raw_first(d)
        for d in (0, 1):
            raw_second(d)
        drain(mrx.at[pl.ds(0, 7)], mrx_sem.at[0])
        second = 8 + here[1] * 4 + here[2]
        mrx[second] = add_up(0, 8)
        for o in plane:
            for c in (0, 1):
                send(mrx.at[second], mrx.at[second], mtx_sem.at[1], mrx_sem.at[1], away(*o, c))
        send(mrx.at[second], mrx.at[second], mtx_sem.at[1], mrx_sem.at[1], partner)
        for d in (2, 3, 4, 5):
            raw_part(d, 1)
        for d in (2, 3, 4, 5):
            raw_second(d)
        drain(mrx.at[pl.ds(8, 15)], mrx_sem.at[1])
        drain(mrx.at[pl.ds(0, 3)], mtx_sem.at[0])
        drain(mrx.at[pl.ds(0, 15)], mtx_sem.at[1])
        drain(mrx.at[pl.ds(0, 16)], mtx_sem.at[1])

    market = add_up(8, 16) / (SER * 128)
    swing = market - jnp.sum(market, axis=1, keepdims=True) / BARS

    def zscore(series):
        deviation = series - swing
        inverse = lax.rsqrt(
            jnp.sum(deviation * deviation, axis=1, keepdims=True) / BARS + 1e-6
        ) / math.sqrt(BARS)
        return (deviation * inverse).astype(jnp.bfloat16)

    def forward(slot, d):
        send(
            zbuf.at[TABLE[slot][d][0]], zbuf.at[2 + 6 * slot + d],
            ztx_sem.at[slot], zrx_sem.at[slot], next_to[d],
        )

    late = pl.ds(QUARTER, QUARTER)
    for half in range(2):
        z = zscore(rt[half * HALF:(half + 1) * HALF])
        zbuf[half] = z
        lhs[half * HALF:(half + 1) * HALF] = z
        for d in range(6):
            if TABLE[1][d][0] == half:
                send(
                    zbuf.at[half, late], zbuf.at[8 + d, late],
                    ztx_sem.at[1], zrx_sem.at[1], next_to[d],
                )
    send(lhs.at[pl.ds(0, SER)], lhs.at[pl.ds(SER, SER)], ltx_sem, lrx_sem, partner)

    drain(raw, wrx_sem)
    waiting = list(PLAN[0])
    for n in range(6):
        zbuf[2 + n] = zscore(raw[n])
        held = set()
        for slot, d in list(waiting):
            if d in held or TABLE[slot][d][0] > 2 + n:
                held.add(d)
            else:
                forward(slot, d)
                waiting.remove((slot, d))
    drain(early, erx_sem)

    def from_early(d, carry):
        zbuf[8 + d, :QUARTER] = zscore(early[d])
        return carry

    lax.fori_loop(0, 6, from_early, 0)

    def tiles(piece, origins, where, send_sem, recv_sem, side=None):
        count = len(origins)
        pieces = zbuf[pl.ds(piece, count)].reshape(count * HALF, BARS)
        rows = slice(None) if side is None else slice(side * SER, (side + 1) * SER)
        both = lax.dot_general(
            lhs[rows], pieces, (((1,), (1,)), ((), ())), preferred_element_type=jnp.float32
        )
        for n, (source, half) in enumerate(origins):
            part = both[:, n * HALF:(n + 1) * HALF]
            column = pl.ds(pl.multiple_of(source * SER + half * HALF, HALF), HALF)
            if side != 0:
                where[n] = jnp.where(source >= theirs, part[-SER:], 0.0).astype(jnp.bfloat16)
                send(where.at[n], out_ref.at[:, column], send_sem, recv_sem, partner)
            if side != 1:
                out_ref[:, column] = jnp.where(source >= mine, part[:SER], 0.0).astype(jnp.bfloat16)

    def landed(slot):
        if slot == 1:
            return zbuf.at[pl.ds(8, 6), late]
        return zbuf.at[pl.ds(2 + 6 * slot, 6)]

    drain(lhs.at[pl.ds(SER, SER)], lrx_sem)
    tiles(0, ((mine, 0), (mine, 1)), stage.at[2, pl.ds(0, 2)], ttx_sem.at[2], trx_sem.at[SLOTS])

    def settle(slot):
        if slot:
            drain(landed(slot), ztx_sem.at[slot])
        drain(stage.at[0], trx_sem.at[slot])

    for slot in range(SLOTS):
        if slot:
            drain(landed(slot), zrx_sem.at[slot])
            for later, d in PLAN[slot]:
                forward(later, d)
        bank = slot % 2
        if slot >= 2:
            drain(stage.at[bank], ttx_sem.at[bank])
        origins = [
            (block([(here[a] + 4 - o[a]) % 4 for a in range(3)], core), h) for _, o, h in TABLE[slot]
        ]
        for side in ((None,) if slot < SLOTS - 1 else (1, 0)):
            tiles(
                2 + 6 * slot, origins, stage.at[bank], ttx_sem.at[bank], trx_sem.at[slot], side
            )
        if slot >= BEHIND:
            settle(slot - BEHIND)

    for slot in range(SLOTS - BEHIND, SLOTS):
        settle(slot)
    drain(stage.at[0], ttx_sem.at[0])
    drain(stage.at[1], ttx_sem.at[1])
    drain(stage.at[2, pl.ds(0, 2)], ttx_sem.at[2])
    drain(stage.at[2, pl.ds(0, 2)], trx_sem.at[SLOTS])
    drain(lhs.at[pl.ds(0, SER)], ltx_sem)
    drain(raw, wtx_sem)
    drain(early, etx_sem)


def write_out(held_ref, out_ref, sem):
    rows = SER // PARTS
    copies = []
    for n in range(PARTS):
        part = pl.ds(n * rows, rows)
        copies.append(pltpu.make_async_copy(held_ref.at[part], out_ref.at[part], sem.at[n]))
        copies[n].start()
    for copy in copies:
        copy.wait()


def shards(returns):
    dma = pltpu.SemaphoreType.DMA
    held = pl.pallas_call(
        kernel,
        out_shape=pltpu.VMEM((SER, 128 * SER), jnp.bfloat16),
        in_specs=[pl.BlockSpec(memory_space=pltpu.HBM)],
        out_specs=pl.BlockSpec(memory_space=pltpu.VMEM),
        scratch_shapes=[
            pltpu.VMEM((128, HALF, BARS), jnp.bfloat16),
            pltpu.VMEM((2 * SER, BARS), jnp.bfloat16),
            pltpu.VMEM((3, 6, SER, HALF), jnp.bfloat16),
            pltpu.VMEM((BARS, SER), jnp.float32),
            pltpu.VMEM((SER, BARS), jnp.float32),
            pltpu.VMEM((6, HALF, BARS), jnp.float32),
            pltpu.VMEM((6, QUARTER, BARS), jnp.float32),
            pltpu.VMEM((24, 1, BARS), jnp.float32),
            dma((CHUNKS,)), dma((2,)), dma((2,)), dma, dma, dma, dma, dma, dma,
            dma((SLOTS,)), dma((SLOTS,)), dma((3,)), dma((SLOTS + 1,)),
        ],
        compiler_params=pltpu.CompilerParams(
            collective_id=0, has_side_effects=True, vmem_limit_bytes=30 * 2**20
        ),
    )(pltpu.with_memory_space_constraint(returns, pltpu.HBM))
    return pl.pallas_call(
        write_out,
        out_shape=jax.ShapeDtypeStruct((SER, 128 * SER), jnp.bfloat16),
        in_specs=[pl.BlockSpec(memory_space=pltpu.VMEM)],
        out_specs=pl.BlockSpec(memory_space=pl.ANY),
        scratch_shapes=[dma((PARTS,))],
        compiler_params=pltpu.CompilerParams(vmem_limit_bytes=2**20),
    )(pltpu.with_memory_space_constraint(held, pltpu.VMEM))


def solution(mesh):
    axes = ("blk", "grp")
    return jax.shard_map(
        shards, mesh=mesh, in_specs=(P(None, axes),), out_specs=P(axes, None), check_vma=False
    )
```

```python
import functools
import math

import jax
import jax.numpy as jnp
from jax import lax
from jax.experimental import pallas as pl
from jax.experimental.pallas import tpu as pltpu
from jax.sharding import PartitionSpec as P

MESH = pl.DeviceIdType.MESH
BARS = 512
SER = 256
HALF = SER // 2
PARTS = 8
DEPTH = 4
BEHIND = 3
QUARTER = HALF // 2
CHUNKS = 4

TREE = [
    [(0, 1), (0, 1), (0, 1)], [(0, -1), (0, -1), (0, -1)], [(1, 1), (1, -1), (4, -1)],
    [(4, 1), (3, -1), (1, 1)], [(48, 1), (3, 1), (12, -1)], [(16, -1), (4, 1), (16, 1)],
    [(17, 1), (16, -1), (3, -1)], [(32, -1), (16, 1), (8, 1)], [(13, 1), (15, -1), (17, 1)],
    [(8, 1), (19, -1), (20, 1)], [(7, -1), (52, 1), (15, -1)], [(52, -1), (17, -1), (13, -1)],
    [(49, 1), (17, 1), (7, 1)], [(52, 1), (18, -1), (28, 1)], [(24, -1), (35, 1), (61, -1)],
    [(36, 1), (63, -1), (24, 1)], [(24, 1), (18, 1), (31, 1)], [(56, 1), (14, -1), (6, -1)],
    [(61, 1), (39, 1), (18, 1)], [(59, -1), (45, -1), (22, 1)], [(43, -1), (30, -1), (30, 1)],
]
SLOTS = len(TREE)


def build():
    place = {(0, 0, 0, 0): 0, (0, 0, 0, 1): 1}
    table = []
    for slot, row in enumerate(TREE):
        line = [None] * 6
        for axis, (parent, sign) in enumerate(row):
            for half in range(2):
                way = sign if half == 0 else -sign
                at = [parent % 4, parent // 4 % 4, parent // 16]
                if half:
                    at = [(-v) % 4 for v in at]
                to = list(at)
                to[axis] = (to[axis] + way) % 4
                d = 2 * axis + (way < 0)
                line[d] = (place[(*at, half)], tuple(to), half)
                place[(*to, half)] = 2 + 6 * slot + d
        table.append(line)
    return table


TABLE = build()


def issue_plan():
    plan = [[] for _ in range(SLOTS)]
    when = [0] * 6
    for slot in range(2, SLOTS):
        for d in range(6):
            when[d] = max((TABLE[slot][d][0] - 2) // 6, when[d], slot - DEPTH)
            plan[when[d]].append((slot, d))
    return plan


PLAN = issue_plan()


def kernel(
    r_ref, out_ref, zbuf, lhs, stage, inp, rt, raw, mrx,
    met, in_sem, mtx_sem, mrx_sem, wtx_sem, wrx_sem, ltx_sem, lrx_sem, ztx_sem, zrx_sem, ttx_sem, trx_sem,
):
    span = BARS // CHUNKS
    loads = []
    for q in range(CHUNKS):
        part = pl.ds(q * span, span)
        loads.append(pltpu.make_async_copy(r_ref.at[part], inp.at[part], in_sem.at[q]))
        loads[q].start()
    blk = lax.axis_index("blk")
    grp = lax.axis_index("grp")
    core = blk % 2
    here = [blk // 8 % 4, blk // 2 % 4, grp * 2 + blk // 32]

    def device(at, c):
        x, y, z = at
        return (((z % 2) * 4 + x) * 4 + y) * 2 + c, z // 2

    def block(at, c):
        b, g = device(at, c)
        return b * 2 + g

    def away(x, y, z, c):
        return device([(here[0] + x) % 4, (here[1] + y) % 4, (here[2] + z) % 4], c)

    mine = block(here, core)
    theirs = block(here, 1 - core)
    partner = device(here, 1 - core)
    steps = [(1, 0, 0), (3, 0, 0), (0, 1, 0), (0, 3, 0), (0, 0, 1), (0, 0, 3)]
    next_to = [away(*step, core) for step in steps]
    ring = [(x, 0, 0) for x in (2, 1, 3)]
    plane = [(0, y, z) for y in (2, 1, 3, 0) for z in (2, 1, 3, 0) if (y, z) != (0, 0)]

    def send(src, dst, send_sem, recv_sem, to):
        pltpu.make_async_remote_copy(
            src_ref=src, dst_ref=dst, send_sem=send_sem, recv_sem=recv_sem,
            device_id=to, device_id_type=MESH,
        ).start()

    def drain(ref, sem):
        pltpu.make_async_copy(ref, ref, sem).wait()

    barrier = pltpu.get_barrier_semaphore()

    def greet(devices):
        for to in devices:
            pl.semaphore_signal(barrier, inc=1, device_id=to, device_id_type=MESH)
        return len(devices)

    around = [partner] + [away(*o, 1 - core) for o in ring]
    axial = [away(*o, 1) for o in plane if 0 in o[1:]]
    over_z = [away(*o, 1) for o in plane if o[1] == 0]

    @pl.when(core == 0)
    def _():
        greet(around + next_to + axial)

    @pl.when(core == 1)
    def _():
        greet(around + [away(*o, core) for o in ring] + axial)

    first = here[0] * 2 + core
    for q in range(CHUNKS):
        loads[q].wait()
        bars = inp[q * span:(q + 1) * span]
        pairs = bars[:, :HALF] + bars[:, HALF:]
        mrx[first, :, q * span:(q + 1) * span] = jnp.sum(pairs.T, axis=0, keepdims=True)

    def add_up(low, count):
        total = mrx[low]
        for n in range(1, count):
            total = total + mrx[low + n]
        return total

    def raw_first(d):
        send(rt.at[pl.ds((d % 2) * HALF, HALF)], raw.at[d], wtx_sem, wrx_sem, next_to[d])

    def turn():
        for q in range(CHUNKS):
            rt[:, q * span:(q + 1) * span] = inp[q * span:(q + 1) * span].T
        series = rt[...]
        rt[...] = series - jnp.sum(series, axis=1, keepdims=True) / BARS

    @pl.when(core == 0)
    def _():
        pl.semaphore_wait(barrier, 4 + 6)
        send(mrx.at[first], mrx.at[first], mtx_sem.at[0], mrx_sem.at[0], partner)
        for o in ring:
            send(mrx.at[first], mrx.at[first], mtx_sem.at[0], mrx_sem.at[0], away(*o, 1))
        turn()
        for d in range(6):
            raw_first(d)
        drain(mrx.at[pl.ds(8, 16)], mrx_sem.at[1])
        drain(mrx.at[pl.ds(0, 4)], mtx_sem.at[0])

    @pl.when(core == 1)
    def _():
        pl.semaphore_wait(barrier, 4 + 3 + 6 + 6)
        for to in over_z:
            pl.semaphore_signal(met, inc=1, device_id=to, device_id_type=MESH)
        for o in ring:
            send(mrx.at[first], mrx.at[first], mtx_sem.at[0], mrx_sem.at[0], away(*o, 1))
        turn()
        for d in (0, 1):
            raw_first(d)
        drain(mrx.at[pl.ds(0, 7)], mrx_sem.at[0])
        second = 8 + here[1] * 4 + here[2]
        pl.semaphore_wait(met, 3)
        mrx[second] = add_up(0, 8)
        for o in plane:
            for c in (0, 1):
                send(mrx.at[second], mrx.at[second], mtx_sem.at[1], mrx_sem.at[1], away(*o, c))
        send(mrx.at[second], mrx.at[second], mtx_sem.at[1], mrx_sem.at[1], partner)
        for d in (2, 3, 4, 5):
            raw_first(d)
        drain(mrx.at[pl.ds(8, 15)], mrx_sem.at[1])
        drain(mrx.at[pl.ds(0, 3)], mtx_sem.at[0])
        drain(mrx.at[pl.ds(0, 15)], mtx_sem.at[1])
        drain(mrx.at[pl.ds(0, 16)], mtx_sem.at[1])

    market = add_up(8, 16) / (SER * 128)
    swing = market - jnp.sum(market, axis=1, keepdims=True) / BARS

    def zscore(series):
        deviation = series - swing
        inverse = lax.rsqrt(
            jnp.sum(deviation * deviation, axis=1, keepdims=True) / BARS + 1e-6
        ) / math.sqrt(BARS)
        return (deviation * inverse).astype(jnp.bfloat16)

    def forward(slot, d):
        send(
            zbuf.at[TABLE[slot][d][0]], zbuf.at[2 + 6 * slot + d],
            ztx_sem.at[slot], zrx_sem.at[slot], next_to[d],
        )

    for half in range(2):
        z = zscore(rt[half * HALF:(half + 1) * HALF])
        zbuf[half] = z
        lhs[half * HALF:(half + 1) * HALF] = z
        for d in range(6):
            if TABLE[1][d][0] == half:
                send(
                    zbuf.at[half], zbuf.at[8 + d],
                    ztx_sem.at[1], zrx_sem.at[1], next_to[d],
                )
    send(lhs.at[pl.ds(0, SER)], lhs.at[pl.ds(SER, SER)], ltx_sem, lrx_sem, partner)

    drain(raw, wrx_sem)
    waiting = list(PLAN[0])
    for n in range(6):
        zbuf[2 + n] = zscore(raw[n])
        held = set()
        for slot, d in list(waiting):
            if d in held or TABLE[slot][d][0] > 2 + n:
                held.add(d)
            else:
                forward(slot, d)
                waiting.remove((slot, d))
    def tiles(piece, origins, where, send_sem, recv_sem, side=None):
        count = len(origins)
        pieces = zbuf[pl.ds(piece, count)].reshape(count * HALF, BARS)
        rows = slice(None) if side is None else slice(side * SER, (side + 1) * SER)
        both = lax.dot_general(
            lhs[rows], pieces, (((1,), (1,)), ((), ())), preferred_element_type=jnp.float32
        )
        for n, (source, half) in enumerate(origins):
            part = both[:, n * HALF:(n + 1) * HALF]
            column = pl.ds(pl.multiple_of(source * SER + half * HALF, HALF), HALF)
            if side != 0:
                where[n] = jnp.where(source >= theirs, part[-SER:], 0.0).astype(jnp.bfloat16)
                send(where.at[n], out_ref.at[:, column], send_sem, recv_sem, partner)
            if side != 1:
                out_ref[:, column] = jnp.where(source >= mine, part[:SER], 0.0).astype(jnp.bfloat16)

    def landed(slot):
        return zbuf.at[pl.ds(2 + 6 * slot, 6)]

    drain(lhs.at[pl.ds(SER, SER)], lrx_sem)
    tiles(0, ((mine, 0), (mine, 1)), stage.at[2, pl.ds(0, 2)], ttx_sem.at[2], trx_sem.at[SLOTS])

    def settle(slot):
        if slot:
            drain(landed(slot), ztx_sem.at[slot])
        drain(stage.at[0], trx_sem.at[slot])

    for slot in range(SLOTS):
        if slot:
            drain(landed(slot), zrx_sem.at[slot])
            for later, d in PLAN[slot]:
                forward(later, d)
        bank = slot % 2
        if slot >= 2:
            drain(stage.at[bank], ttx_sem.at[bank])
        origins = [
            (block([(here[a] + 4 - o[a]) % 4 for a in range(3)], core), h) for _, o, h in TABLE[slot]
        ]
        for side in ((None,) if slot < SLOTS - 1 else (1, 0)):
            tiles(
                2 + 6 * slot, origins, stage.at[bank], ttx_sem.at[bank], trx_sem.at[slot], side
            )
        if slot >= BEHIND:
            settle(slot - BEHIND)

    for slot in range(SLOTS - BEHIND, SLOTS):
        settle(slot)
    drain(stage.at[0], ttx_sem.at[0])
    drain(stage.at[1], ttx_sem.at[1])
    drain(stage.at[2, pl.ds(0, 2)], ttx_sem.at[2])
    drain(stage.at[2, pl.ds(0, 2)], trx_sem.at[SLOTS])
    drain(lhs.at[pl.ds(0, SER)], ltx_sem)
    drain(raw, wtx_sem)


def write_out(held_ref, out_ref, sem):
    rows = SER // PARTS
    copies = []
    for n in range(PARTS):
        part = pl.ds(n * rows, rows)
        copies.append(pltpu.make_async_copy(held_ref.at[part], out_ref.at[part], sem.at[n]))
        copies[n].start()
    for copy in copies:
        copy.wait()


def shards(returns):
    dma = pltpu.SemaphoreType.DMA
    held = pl.pallas_call(
        kernel,
        out_shape=pltpu.VMEM((SER, 128 * SER), jnp.bfloat16),
        in_specs=[pl.BlockSpec(memory_space=pltpu.HBM)],
        out_specs=pl.BlockSpec(memory_space=pltpu.VMEM),
        scratch_shapes=[
            pltpu.VMEM((128, HALF, BARS), jnp.bfloat16),
            pltpu.VMEM((2 * SER, BARS), jnp.bfloat16),
            pltpu.VMEM((3, 6, SER, HALF), jnp.bfloat16),
            pltpu.VMEM((BARS, SER), jnp.float32),
            pltpu.VMEM((SER, BARS), jnp.float32),
            pltpu.VMEM((6, HALF, BARS), jnp.float32),
            pltpu.VMEM((24, 1, BARS), jnp.float32),
            pltpu.SemaphoreType.REGULAR, dma((CHUNKS,)), dma((2,)), dma((2,)), dma, dma, dma, dma,
            dma((SLOTS,)), dma((SLOTS,)), dma((3,)), dma((SLOTS + 1,)),
        ],
        compiler_params=pltpu.CompilerParams(
            collective_id=0, has_side_effects=True, vmem_limit_bytes=30 * 2**20
        ),
    )(pltpu.with_memory_space_constraint(returns, pltpu.HBM))
    return pl.pallas_call(
        write_out,
        out_shape=jax.ShapeDtypeStruct((SER, 128 * SER), jnp.bfloat16),
        in_specs=[pl.BlockSpec(memory_space=pltpu.VMEM)],
        out_specs=pl.BlockSpec(memory_space=pl.ANY),
        scratch_shapes=[dma((PARTS,))],
        compiler_params=pltpu.CompilerParams(vmem_limit_bytes=2**20),
    )(pltpu.with_memory_space_constraint(held, pltpu.VMEM))


def solution(mesh):
    axes = ("blk", "grp")
    return jax.shard_map(
        shards, mesh=mesh, in_specs=(P(None, axes),), out_specs=P(axes, None), check_vma=False
    )
```

```python
import functools
import math

import jax
import jax.numpy as jnp
from jax import lax
from jax.experimental import pallas as pl
from jax.experimental.pallas import tpu as pltpu
from jax.sharding import PartitionSpec as P

MESH = pl.DeviceIdType.MESH
BARS = 512
SER = 256
HALF = SER // 2
PARTS = 8
DEPTH = 4
BEHIND = 3
QUARTER = HALF // 2
CHUNKS = 4

TREE = [
    [(0, 1), (0, 1), (0, 1)], [(0, -1), (0, -1), (0, -1)], [(16, 1), (16, -1), (4, 1)],
    [(48, 1), (1, 1), (12, -1)], [(4, -1), (4, 1), (3, -1)], [(1, 1), (48, 1), (48, -1)],
    [(12, 1), (3, -1), (20, 1)], [(60, -1), (7, 1), (3, 1)], [(52, -1), (17, 1), (7, 1)],
    [(51, -1), (49, -1), (8, 1)], [(17, 1), (19, -1), (5, -1)], [(28, 1), (2, -1), (51, -1)],
    [(5, 1), (32, -1), (8, -1)], [(23, -1), (13, -1), (49, -1)], [(36, 1), (36, 1), (63, -1)],
    [(63, -1), (61, -1), (55, -1)], [(24, -1), (21, 1), (50, -1)], [(40, -1), (14, -1), (11, -1)],
    [(29, 1), (50, 1), (61, -1)], [(57, 1), (37, 1), (22, 1)], [(43, -1), (34, -1), (10, 1)],
]
SLOTS = len(TREE)


def build():
    place = {(0, 0, 0, 0): 0, (0, 0, 0, 1): 1}
    table = []
    for slot, row in enumerate(TREE):
        line = [None] * 6
        for axis, (parent, sign) in enumerate(row):
            for half in range(2):
                way = sign if half == 0 else -sign
                at = [parent % 4, parent // 4 % 4, parent // 16]
                if half:
                    at = [(-v) % 4 for v in at]
                to = list(at)
                to[axis] = (to[axis] + way) % 4
                d = 2 * axis + (way < 0)
                line[d] = (place[(*at, half)], tuple(to), half)
                place[(*to, half)] = 2 + 6 * slot + d
        table.append(line)
    return table


TABLE = build()


def issue_plan():
    plan = [[] for _ in range(SLOTS)]
    when = [0] * 6
    for slot in range(2, SLOTS):
        for d in range(6):
            when[d] = max((TABLE[slot][d][0] - 2) // 6, when[d], slot - DEPTH)
            plan[when[d]].append((slot, d))
    return plan


PLAN = issue_plan()


def kernel(
    r_ref, out_ref, zbuf, lhs, stage, inp, rt, raw, mrx,
    met, in_sem, mtx_sem, mrx_sem, wtx_sem, wrx_sem, ltx_sem, lrx_sem, ztx_sem, zrx_sem, ttx_sem, trx_sem,
):
    span = BARS // CHUNKS
    loads = []
    for q in range(CHUNKS):
        part = pl.ds(q * span, span)
        loads.append(pltpu.make_async_copy(r_ref.at[part], inp.at[part], in_sem.at[q]))
        loads[q].start()
    blk = lax.axis_index("blk")
    grp = lax.axis_index("grp")
    core = blk % 2
    here = [blk // 8 % 4, blk // 2 % 4, grp * 2 + blk // 32]

    def device(at, c):
        x, y, z = at
        return (((z % 2) * 4 + x) * 4 + y) * 2 + c, z // 2

    def block(at, c):
        b, g = device(at, c)
        return b * 2 + g

    def away(x, y, z, c):
        return device([(here[0] + x) % 4, (here[1] + y) % 4, (here[2] + z) % 4], c)

    mine = block(here, core)
    theirs = block(here, 1 - core)
    partner = device(here, 1 - core)
    steps = [(1, 0, 0), (3, 0, 0), (0, 1, 0), (0, 3, 0), (0, 0, 1), (0, 0, 3)]
    next_to = [away(*step, core) for step in steps]
    ring = [(x, 0, 0) for x in (2, 1, 3)]
    plane = [(0, y, z) for y in (2, 1, 3, 0) for z in (2, 1, 3, 0) if (y, z) != (0, 0)]

    def send(src, dst, send_sem, recv_sem, to):
        pltpu.make_async_remote_copy(
            src_ref=src, dst_ref=dst, send_sem=send_sem, recv_sem=recv_sem,
            device_id=to, device_id_type=MESH,
        ).start()

    def drain(ref, sem):
        pltpu.make_async_copy(ref, ref, sem).wait()

    barrier = pltpu.get_barrier_semaphore()

    def greet(devices):
        for to in devices:
            pl.semaphore_signal(barrier, inc=1, device_id=to, device_id_type=MESH)
        return len(devices)

    around = [partner] + [away(*o, 1 - core) for o in ring]
    axial = [away(*o, 1) for o in plane if 0 in o[1:]]
    over_z = [away(*o, 1) for o in plane if o[1] == 0]

    @pl.when(core == 0)
    def _():
        greet(around + next_to + axial)

    @pl.when(core == 1)
    def _():
        greet(around + [away(*o, core) for o in ring] + axial)

    first = here[0] * 2 + core
    for q in range(CHUNKS):
        loads[q].wait()
        bars = inp[q * span:(q + 1) * span]
        pairs = bars[:, :HALF] + bars[:, HALF:]
        mrx[first, :, q * span:(q + 1) * span] = jnp.sum(pairs.T, axis=0, keepdims=True)

    def add_up(low, count):
        total = mrx[low]
        for n in range(1, count):
            total = total + mrx[low + n]
        return total

    def raw_first(d):
        send(rt.at[pl.ds((d % 2) * HALF, HALF)], raw.at[d], wtx_sem, wrx_sem, next_to[d])

    def turn():
        for q in range(CHUNKS):
            rt[:, q * span:(q + 1) * span] = inp[q * span:(q + 1) * span].T
        series = rt[...]
        rt[...] = series - jnp.sum(series, axis=1, keepdims=True) / BARS

    @pl.when(core == 0)
    def _():
        pl.semaphore_wait(barrier, 4 + 6)
        send(mrx.at[first], mrx.at[first], mtx_sem.at[0], mrx_sem.at[0], partner)
        for o in ring:
            send(mrx.at[first], mrx.at[first], mtx_sem.at[0], mrx_sem.at[0], away(*o, 1))
        turn()
        for d in range(6):
            raw_first(d)
        drain(mrx.at[pl.ds(8, 16)], mrx_sem.at[1])
        drain(mrx.at[pl.ds(0, 4)], mtx_sem.at[0])

    @pl.when(core == 1)
    def _():
        pl.semaphore_wait(barrier, 4 + 3 + 6 + 6)
        for to in over_z:
            pl.semaphore_signal(met, inc=1, device_id=to, device_id_type=MESH)
        for o in ring:
            send(mrx.at[first], mrx.at[first], mtx_sem.at[0], mrx_sem.at[0], away(*o, 1))
        turn()
        for d in (0, 1):
            raw_first(d)
        drain(mrx.at[pl.ds(0, 7)], mrx_sem.at[0])
        second = 8 + here[1] * 4 + here[2]
        pl.semaphore_wait(met, 3)
        mrx[second] = add_up(0, 8)
        for o in plane:
            for c in (0, 1):
                send(mrx.at[second], mrx.at[second], mtx_sem.at[1], mrx_sem.at[1], away(*o, c))
        send(mrx.at[second], mrx.at[second], mtx_sem.at[1], mrx_sem.at[1], partner)
        for d in (2, 3, 4, 5):
            raw_first(d)
        drain(mrx.at[pl.ds(8, 15)], mrx_sem.at[1])
        drain(mrx.at[pl.ds(0, 3)], mtx_sem.at[0])
        drain(mrx.at[pl.ds(0, 15)], mtx_sem.at[1])
        drain(mrx.at[pl.ds(0, 16)], mtx_sem.at[1])

    market = add_up(8, 16) / (SER * 128)
    swing = market - jnp.sum(market, axis=1, keepdims=True) / BARS

    def zscore(series):
        deviation = series - swing
        inverse = lax.rsqrt(
            jnp.sum(deviation * deviation, axis=1, keepdims=True) / BARS + 1e-6
        ) / math.sqrt(BARS)
        return (deviation * inverse).astype(jnp.bfloat16)

    def forward(slot, d):
        send(
            zbuf.at[TABLE[slot][d][0]], zbuf.at[2 + 6 * slot + d],
            ztx_sem.at[slot], zrx_sem.at[slot], next_to[d],
        )

    for half in range(2):
        z = zscore(rt[half * HALF:(half + 1) * HALF])
        zbuf[half] = z
        lhs[half * HALF:(half + 1) * HALF] = z
        for d in range(6):
            if TABLE[1][d][0] == half:
                send(
                    zbuf.at[half], zbuf.at[8 + d],
                    ztx_sem.at[1], zrx_sem.at[1], next_to[d],
                )
    send(lhs.at[pl.ds(0, SER)], lhs.at[pl.ds(SER, SER)], ltx_sem, lrx_sem, partner)

    drain(raw, wrx_sem)
    waiting = list(PLAN[0])
    for n in range(6):
        zbuf[2 + n] = zscore(raw[n])
        held = set()
        for slot, d in list(waiting):
            if d in held or TABLE[slot][d][0] > 2 + n:
                held.add(d)
            else:
                forward(slot, d)
                waiting.remove((slot, d))
    def tiles(piece, origins, where, send_sem, recv_sem, side=None):
        count = len(origins)
        pieces = zbuf[pl.ds(piece, count)].reshape(count * HALF, BARS)
        rows = slice(None) if side is None else slice(side * SER, (side + 1) * SER)
        both = lax.dot_general(
            lhs[rows], pieces, (((1,), (1,)), ((), ())), preferred_element_type=jnp.float32
        )
        for n, (source, half) in enumerate(origins):
            part = both[:, n * HALF:(n + 1) * HALF]
            column = pl.ds(pl.multiple_of(source * SER + half * HALF, HALF), HALF)
            if side != 0:
                where[n] = jnp.where(source >= theirs, part[-SER:], 0.0).astype(jnp.bfloat16)
                send(where.at[n], out_ref.at[:, column], send_sem, recv_sem, partner)
            if side != 1:
                out_ref[:, column] = jnp.where(source >= mine, part[:SER], 0.0).astype(jnp.bfloat16)

    def landed(slot):
        return zbuf.at[pl.ds(2 + 6 * slot, 6)]

    drain(lhs.at[pl.ds(SER, SER)], lrx_sem)
    tiles(0, ((mine, 0), (mine, 1)), stage.at[2, pl.ds(0, 2)], ttx_sem.at[2], trx_sem.at[SLOTS])

    def settle(slot):
        if slot:
            drain(landed(slot), ztx_sem.at[slot])
        drain(stage.at[0], trx_sem.at[slot])

    for slot in range(SLOTS):
        if slot:
            drain(landed(slot), zrx_sem.at[slot])
            for later, d in PLAN[slot]:
                forward(later, d)
        bank = slot % 2
        if slot >= 2:
            drain(stage.at[bank], ttx_sem.at[bank])
        origins = [
            (block([(here[a] + 4 - o[a]) % 4 for a in range(3)], core), h) for _, o, h in TABLE[slot]
        ]
        for side in ((None,) if slot < SLOTS - 1 else (1, 0)):
            tiles(
                2 + 6 * slot, origins, stage.at[bank], ttx_sem.at[bank], trx_sem.at[slot], side
            )
        if slot >= BEHIND:
            settle(slot - BEHIND)

    for slot in range(SLOTS - BEHIND, SLOTS):
        settle(slot)
    drain(stage.at[0], ttx_sem.at[0])
    drain(stage.at[1], ttx_sem.at[1])
    drain(stage.at[2, pl.ds(0, 2)], ttx_sem.at[2])
    drain(stage.at[2, pl.ds(0, 2)], trx_sem.at[SLOTS])
    drain(lhs.at[pl.ds(0, SER)], ltx_sem)
    drain(raw, wtx_sem)


def write_out(held_ref, out_ref, sem):
    rows = SER // PARTS
    copies = []
    for n in range(PARTS):
        part = pl.ds(n * rows, rows)
        copies.append(pltpu.make_async_copy(held_ref.at[part], out_ref.at[part], sem.at[n]))
        copies[n].start()
    for copy in copies:
        copy.wait()


def shards(returns):
    dma = pltpu.SemaphoreType.DMA
    held = pl.pallas_call(
        kernel,
        out_shape=pltpu.VMEM((SER, 128 * SER), jnp.bfloat16),
        in_specs=[pl.BlockSpec(memory_space=pltpu.HBM)],
        out_specs=pl.BlockSpec(memory_space=pltpu.VMEM),
        scratch_shapes=[
            pltpu.VMEM((128, HALF, BARS), jnp.bfloat16),
            pltpu.VMEM((2 * SER, BARS), jnp.bfloat16),
            pltpu.VMEM((3, 6, SER, HALF), jnp.bfloat16),
            pltpu.VMEM((BARS, SER), jnp.float32),
            pltpu.VMEM((SER, BARS), jnp.float32),
            pltpu.VMEM((6, HALF, BARS), jnp.float32),
            pltpu.VMEM((24, 1, BARS), jnp.float32),
            pltpu.SemaphoreType.REGULAR, dma((CHUNKS,)), dma((2,)), dma((2,)), dma, dma, dma, dma,
            dma((SLOTS,)), dma((SLOTS,)), dma((3,)), dma((SLOTS + 1,)),
        ],
        compiler_params=pltpu.CompilerParams(
            collective_id=0, has_side_effects=True, vmem_limit_bytes=30 * 2**20
        ),
    )(pltpu.with_memory_space_constraint(returns, pltpu.HBM))
    return pl.pallas_call(
        write_out,
        out_shape=jax.ShapeDtypeStruct((SER, 128 * SER), jnp.bfloat16),
        in_specs=[pl.BlockSpec(memory_space=pltpu.VMEM)],
        out_specs=pl.BlockSpec(memory_space=pl.ANY),
        scratch_shapes=[dma((PARTS,))],
        compiler_params=pltpu.CompilerParams(vmem_limit_bytes=2**20),
    )(pltpu.with_memory_space_constraint(held, pltpu.VMEM))


def solution(mesh):
    axes = ("blk", "grp")
    return jax.shard_map(
        shards, mesh=mesh, in_specs=(P(None, axes),), out_specs=P(axes, None), check_vma=False
    )
```

```python
import functools
import math

import jax
import jax.numpy as jnp
from jax import lax
from jax.experimental import pallas as pl
from jax.experimental.pallas import tpu as pltpu
from jax.sharding import PartitionSpec as P

MESH = pl.DeviceIdType.MESH
BARS = 512
SER = 256
HALF = SER // 2
PARTS = 8
DEPTH = 6
BEHIND = 3
QUARTER = HALF // 2
CHUNKS = 4

TREE = [
    [(0, 1), (0, 1), (0, 1)], [(0, -1), (0, -1), (0, -1)], [(16, 1), (16, -1), (4, 1)],
    [(48, 1), (1, 1), (12, -1)], [(4, -1), (4, 1), (3, -1)], [(1, 1), (48, 1), (48, -1)],
    [(12, 1), (3, -1), (20, 1)], [(60, -1), (7, 1), (3, 1)], [(52, -1), (17, 1), (7, 1)],
    [(51, -1), (49, -1), (8, 1)], [(17, 1), (19, -1), (5, -1)], [(28, 1), (2, -1), (51, -1)],
    [(5, 1), (32, -1), (8, -1)], [(23, -1), (13, -1), (49, -1)], [(36, 1), (36, 1), (63, -1)],
    [(63, -1), (61, -1), (55, -1)], [(24, -1), (21, 1), (50, -1)], [(40, -1), (14, -1), (11, -1)],
    [(29, 1), (50, 1), (61, -1)], [(57, 1), (37, 1), (22, 1)], [(43, -1), (34, -1), (10, 1)],
]
SLOTS = len(TREE)


def build():
    place = {(0, 0, 0, 0): 0, (0, 0, 0, 1): 1}
    table = []
    for slot, row in enumerate(TREE):
        line = [None] * 6
        for axis, (parent, sign) in enumerate(row):
            for half in range(2):
                way = sign if half == 0 else -sign
                at = [parent % 4, parent // 4 % 4, parent // 16]
                if half:
                    at = [(-v) % 4 for v in at]
                to = list(at)
                to[axis] = (to[axis] + way) % 4
                d = 2 * axis + (way < 0)
                line[d] = (place[(*at, half)], tuple(to), half)
                place[(*to, half)] = 2 + 6 * slot + d
        table.append(line)
    return table


TABLE = build()


def issue_plan():
    plan = [[] for _ in range(SLOTS)]
    when = [0] * 6
    for slot in range(2, SLOTS):
        for d in range(6):
            when[d] = max((TABLE[slot][d][0] - 2) // 6, when[d], slot - DEPTH)
            plan[when[d]].append((slot, d))
    return plan


PLAN = issue_plan()


def kernel(
    r_ref, out_ref, zbuf, lhs, stage, inp, rt, raw, mrx,
    met, in_sem, mtx_sem, mrx_sem, wtx_sem, wrx_sem, ltx_sem, lrx_sem, ztx_sem, zrx_sem, ttx_sem, trx_sem,
):
    span = BARS // CHUNKS
    loads = []
    for q in range(CHUNKS):
        part = pl.ds(q * span, span)
        loads.append(pltpu.make_async_copy(r_ref.at[part], inp.at[part], in_sem.at[q]))
        loads[q].start()
    blk = lax.axis_index("blk")
    grp = lax.axis_index("grp")
    core = blk % 2
    here = [blk // 8 % 4, blk // 2 % 4, grp * 2 + blk // 32]

    def device(at, c):
        x, y, z = at
        return (((z % 2) * 4 + x) * 4 + y) * 2 + c, z // 2

    def block(at, c):
        b, g = device(at, c)
        return b * 2 + g

    def away(x, y, z, c):
        return device([(here[0] + x) % 4, (here[1] + y) % 4, (here[2] + z) % 4], c)

    mine = block(here, core)
    theirs = block(here, 1 - core)
    partner = device(here, 1 - core)
    steps = [(1, 0, 0), (3, 0, 0), (0, 1, 0), (0, 3, 0), (0, 0, 1), (0, 0, 3)]
    next_to = [away(*step, core) for step in steps]
    ring = [(x, 0, 0) for x in (2, 1, 3)]
    plane = [(0, y, z) for y in (2, 1, 3, 0) for z in (2, 1, 3, 0) if (y, z) != (0, 0)]

    def send(src, dst, send_sem, recv_sem, to):
        pltpu.make_async_remote_copy(
            src_ref=src, dst_ref=dst, send_sem=send_sem, recv_sem=recv_sem,
            device_id=to, device_id_type=MESH,
        ).start()

    def drain(ref, sem):
        pltpu.make_async_copy(ref, ref, sem).wait()

    barrier = pltpu.get_barrier_semaphore()

    def greet(devices):
        for to in devices:
            pl.semaphore_signal(barrier, inc=1, device_id=to, device_id_type=MESH)
        return len(devices)

    around = [partner] + [away(*o, 1 - core) for o in ring]
    axial = [away(*o, 1) for o in plane if 0 in o[1:]]
    over_z = [away(*o, 1) for o in plane if o[1] == 0]

    @pl.when(core == 0)
    def _():
        greet(around + next_to + axial)

    @pl.when(core == 1)
    def _():
        greet(around + [away(*o, core) for o in ring] + axial)

    first = here[0] * 2 + core
    for q in range(CHUNKS):
        loads[q].wait()
        bars = inp[q * span:(q + 1) * span]
        pairs = bars[:, :HALF] + bars[:, HALF:]
        mrx[first, :, q * span:(q + 1) * span] = jnp.sum(pairs.T, axis=0, keepdims=True)

    def add_up(low, count):
        total = mrx[low]
        for n in range(1, count):
            total = total + mrx[low + n]
        return total

    def raw_first(d):
        send(rt.at[pl.ds((d % 2) * HALF, HALF)], raw.at[d], wtx_sem, wrx_sem, next_to[d])

    def turn():
        for q in range(CHUNKS):
            rt[:, q * span:(q + 1) * span] = inp[q * span:(q + 1) * span].T
        series = rt[...]
        rt[...] = series - jnp.sum(series, axis=1, keepdims=True) / BARS

    @pl.when(core == 0)
    def _():
        pl.semaphore_wait(barrier, 4 + 6)
        send(mrx.at[first], mrx.at[first], mtx_sem.at[0], mrx_sem.at[0], partner)
        for o in ring:
            send(mrx.at[first], mrx.at[first], mtx_sem.at[0], mrx_sem.at[0], away(*o, 1))
        turn()
        for d in range(6):
            raw_first(d)
        drain(mrx.at[pl.ds(8, 16)], mrx_sem.at[1])
        drain(mrx.at[pl.ds(0, 4)], mtx_sem.at[0])

    @pl.when(core == 1)
    def _():
        pl.semaphore_wait(barrier, 4 + 3 + 6 + 6)
        for to in over_z:
            pl.semaphore_signal(met, inc=1, device_id=to, device_id_type=MESH)
        for o in ring:
            send(mrx.at[first], mrx.at[first], mtx_sem.at[0], mrx_sem.at[0], away(*o, 1))
        turn()
        for d in (0, 1):
            raw_first(d)
        drain(mrx.at[pl.ds(0, 7)], mrx_sem.at[0])
        second = 8 + here[1] * 4 + here[2]
        pl.semaphore_wait(met, 3)
        mrx[second] = add_up(0, 8)
        for c in (1, 0):
            for o in plane:
                send(mrx.at[second], mrx.at[second], mtx_sem.at[1], mrx_sem.at[1], away(*o, c))
        send(mrx.at[second], mrx.at[second], mtx_sem.at[1], mrx_sem.at[1], partner)
        for d in (2, 3, 4, 5):
            raw_first(d)
        drain(mrx.at[pl.ds(8, 15)], mrx_sem.at[1])
        drain(mrx.at[pl.ds(0, 3)], mtx_sem.at[0])
        drain(mrx.at[pl.ds(0, 15)], mtx_sem.at[1])
        drain(mrx.at[pl.ds(0, 16)], mtx_sem.at[1])

    market = add_up(8, 16) / (SER * 128)
    swing = market - jnp.sum(market, axis=1, keepdims=True) / BARS

    def zscore(series):
        deviation = series - swing
        inverse = lax.rsqrt(
            jnp.sum(deviation * deviation, axis=1, keepdims=True) / BARS + 1e-6
        ) / math.sqrt(BARS)
        return (deviation * inverse).astype(jnp.bfloat16)

    def forward(slot, d):
        send(
            zbuf.at[TABLE[slot][d][0]], zbuf.at[2 + 6 * slot + d],
            ztx_sem.at[slot], zrx_sem.at[slot], next_to[d],
        )

    for half in range(2):
        z = zscore(rt[half * HALF:(half + 1) * HALF])
        zbuf[half] = z
        lhs[half * HALF:(half + 1) * HALF] = z
        for d in range(6):
            if TABLE[1][d][0] == half:
                send(
                    zbuf.at[half], zbuf.at[8 + d],
                    ztx_sem.at[1], zrx_sem.at[1], next_to[d],
                )
    send(lhs.at[pl.ds(0, SER)], lhs.at[pl.ds(SER, SER)], ltx_sem, lrx_sem, partner)

    drain(raw, wrx_sem)
    waiting = list(PLAN[0])
    for n in range(6):
        zbuf[2 + n] = zscore(raw[n])
        held = set()
        for slot, d in list(waiting):
            if d in held or TABLE[slot][d][0] > 2 + n:
                held.add(d)
            else:
                forward(slot, d)
                waiting.remove((slot, d))
    def tiles(piece, origins, where, send_sem, recv_sem, side=None):
        count = len(origins)
        pieces = zbuf[pl.ds(piece, count)].reshape(count * HALF, BARS)
        rows = slice(None) if side is None else slice(side * SER, (side + 1) * SER)
        both = lax.dot_general(
            lhs[rows], pieces, (((1,), (1,)), ((), ())), preferred_element_type=jnp.float32
        )
        for n, (source, half) in enumerate(origins):
            part = both[:, n * HALF:(n + 1) * HALF]
            column = pl.ds(pl.multiple_of(source * SER + half * HALF, HALF), HALF)
            if side != 0:
                where[n] = jnp.where(source >= theirs, part[-SER:], 0.0).astype(jnp.bfloat16)
                send(where.at[n], out_ref.at[:, column], send_sem, recv_sem, partner)
            if side != 1:
                out_ref[:, column] = jnp.where(source >= mine, part[:SER], 0.0).astype(jnp.bfloat16)

    def landed(slot):
        return zbuf.at[pl.ds(2 + 6 * slot, 6)]

    drain(lhs.at[pl.ds(SER, SER)], lrx_sem)
    tiles(0, ((mine, 0), (mine, 1)), stage.at[2, pl.ds(0, 2)], ttx_sem.at[2], trx_sem.at[SLOTS])

    def settle(slot):
        if slot:
            drain(landed(slot), ztx_sem.at[slot])
        drain(stage.at[0], trx_sem.at[slot])

    for slot in range(SLOTS):
        if slot:
            drain(landed(slot), zrx_sem.at[slot])
            for later, d in PLAN[slot]:
                forward(later, d)
        bank = slot % 2
        if slot >= 2:
            drain(stage.at[bank], ttx_sem.at[bank])
        origins = [
            (block([(here[a] + 4 - o[a]) % 4 for a in range(3)], core), h) for _, o, h in TABLE[slot]
        ]
        for side in ((None,) if slot < SLOTS - 1 else (1, 0)):
            tiles(
                2 + 6 * slot, origins, stage.at[bank], ttx_sem.at[bank], trx_sem.at[slot], side
            )
        if slot >= BEHIND:
            settle(slot - BEHIND)

    for slot in range(SLOTS - BEHIND, SLOTS):
        settle(slot)
    drain(stage.at[0], ttx_sem.at[0])
    drain(stage.at[1], ttx_sem.at[1])
    drain(stage.at[2, pl.ds(0, 2)], ttx_sem.at[2])
    drain(stage.at[2, pl.ds(0, 2)], trx_sem.at[SLOTS])
    drain(lhs.at[pl.ds(0, SER)], ltx_sem)
    drain(raw, wtx_sem)


def write_out(held_ref, out_ref, sem):
    rows = SER // PARTS
    copies = []
    for n in range(PARTS):
        part = pl.ds(n * rows, rows)
        copies.append(pltpu.make_async_copy(held_ref.at[part], out_ref.at[part], sem.at[n]))
        copies[n].start()
    for copy in copies:
        copy.wait()


def shards(returns):
    dma = pltpu.SemaphoreType.DMA
    held = pl.pallas_call(
        kernel,
        out_shape=pltpu.VMEM((SER, 128 * SER), jnp.bfloat16),
        in_specs=[pl.BlockSpec(memory_space=pltpu.HBM)],
        out_specs=pl.BlockSpec(memory_space=pltpu.VMEM),
        scratch_shapes=[
            pltpu.VMEM((128, HALF, BARS), jnp.bfloat16),
            pltpu.VMEM((2 * SER, BARS), jnp.bfloat16),
            pltpu.VMEM((3, 6, SER, HALF), jnp.bfloat16),
            pltpu.VMEM((BARS, SER), jnp.float32),
            pltpu.VMEM((SER, BARS), jnp.float32),
            pltpu.VMEM((6, HALF, BARS), jnp.float32),
            pltpu.VMEM((24, 1, BARS), jnp.float32),
            pltpu.SemaphoreType.REGULAR, dma((CHUNKS,)), dma((2,)), dma((2,)), dma, dma, dma, dma,
            dma((SLOTS,)), dma((SLOTS,)), dma((3,)), dma((SLOTS + 1,)),
        ],
        compiler_params=pltpu.CompilerParams(
            collective_id=0, has_side_effects=True, vmem_limit_bytes=30 * 2**20
        ),
    )(pltpu.with_memory_space_constraint(returns, pltpu.HBM))
    return pl.pallas_call(
        write_out,
        out_shape=jax.ShapeDtypeStruct((SER, 128 * SER), jnp.bfloat16),
        in_specs=[pl.BlockSpec(memory_space=pltpu.VMEM)],
        out_specs=pl.BlockSpec(memory_space=pl.ANY),
        scratch_shapes=[dma((PARTS,))],
        compiler_params=pltpu.CompilerParams(vmem_limit_bytes=2**20),
    )(pltpu.with_memory_space_constraint(held, pltpu.VMEM))


def solution(mesh):
    axes = ("blk", "grp")
    return jax.shard_map(
        shards, mesh=mesh, in_specs=(P(None, axes),), out_specs=P(axes, None), check_vma=False
    )
```
